512 devices in a mesh: ket: 128 (over z, y, core), blk: 4 (over x).
Axes of the slice: x: 4, y: 8, z: 8, core: 2. Of those that a mesh axis runs over, the one named last changes fastest.
Arguments:
- density: float32 [8192, 64, 128], P('ket', 'blk'), may hold values from -24 to 24
- decay_matrix: float32 [128, 128], replicated, may hold values from -0.25 to 2, as said below
- atom_order: int32 [128], replicated, may hold values from 0 to 127, each once
Outputs:
- next_vector: float32 [8192, 64, 128], P('ket', 'blk')
- krylov_coeffs: float32 [5], replicated
- jump_flux: float32 [8192], P(('ket', 'blk'))
The draws below stay inside these ranges and needn't reach their ends.
Inputs may be any that keep to these rules, and one draw needn't show every extreme that they name: `decay_matrix`: symmetric; diagonal entries from 0.5 to 2, off-diagonal entries at most 0.25 in magnitude. `atom_order`: each atom once.
All inputs are finite; a program needn't handle non-finite values.
Results may differ from the reference program's by a relative error of at most 0.0003.
Values sent between devices are 32-bit elements; how exact they have to be, the bound alone decides.
No kernel may reach another device: no remote copies, remote signals or barrier semaphores. Data moves between devices by JAX's collectives and lax.ppermute only.
A program may use at most 64 MiB of HBM per device.

```python
import math
import jax
import jax.numpy as jnp
from jax import lax

N = 128
H = 64
P_SIZE = 8192


def draw_decay_matrix(key, part):
    base = jax.random.fold_in(key, 11)
    first_key, second_key = jax.random.split(base)
    diagonal = jnp.exp(jax.random.uniform(first_key, (N,), jnp.float32, math.log(0.5), math.log(2.0)))
    spread = 0.35
    diagonal = jnp.clip(diagonal, 0.5, 2.0)
    normals = jax.random.normal(second_key, (N, N), jnp.float32)
    offdiag = jnp.clip((normals + normals.T) * (spread / math.sqrt(N)), -0.25, 0.25)
    identity = jnp.arange(N)[:, None] == jnp.arange(N)[None, :]
    return jnp.where(identity, diagonal[:, None], offdiag).astype(jnp.float32)


def strengthened(values, rng, source, target, parts, factor):
    def block_of(axis_at):
        return (jnp.arange(values.shape[axis_at]) // (values.shape[axis_at] // parts)).reshape((-1,) + (1,) * (values.ndim - 1 - axis_at))

    one_side = jax.random.permutation(rng, parts)[block_of(target)]
    second = (block_of(target) + parts // 2) % parts
    return jnp.where((block_of(source) == one_side) | (block_of(source) == second), factor * values, values)


def level_of(rng, shape, cuts, smallest, high):
    loudness, own = 1.0, jax.random.fold_in(rng, 6)
    for dim, shards_of in cuts:
        heights = jnp.exp(jax.random.uniform(jax.random.fold_in(own, dim), (shards_of,), jnp.float32, smallest / len(cuts), high / len(cuts)))
        loudness = loudness * jnp.repeat(heights, shape[dim] // shards_of).reshape([-1 if axis == dim else 1 for axis in range(len(shape))])
    return loudness


def noise_with(own_key, dims, width, bound, pieces, heavy, kind=jnp.bfloat16):
    values = width * jax.random.normal(own_key, dims, jnp.float32)
    if pieces:
        values = values * level_of(own_key, dims, pieces, -0.22, 0.18)
    return jnp.clip(strengthened(values, jax.random.fold_in(own_key, 3), *heavy), -bound, bound).astype(kind)


def setup_inputs(seed: int = 0) -> dict:
    arg_keys = jax.random.split(jax.random.key(seed), 4)
    return {
        "density": noise_with(arg_keys[0], (P_SIZE, H, N), 1.0, 24.0, ((0, 128), (1, 4)), (0, 2, 128, 5.5), jnp.float32),
        "decay_matrix": draw_decay_matrix(jax.random.fold_in(arg_keys[3], 71), 0),
        "atom_order": jax.random.permutation(arg_keys[2], N).astype(jnp.int32),
    }


highest = lax.Precision.HIGHEST

def liouvillian(tensor, coupling):
    atom_count = coupling.shape[0]
    half = tensor.shape[1]
    window = coupling[:half, :half]
    leading = jnp.dot(coupling, tensor.reshape(atom_count, -1), precision=highest).reshape(tensor.shape)
    ket_slabs = tensor.reshape(atom_count, half, half, atom_count)

    def slab_terms(ket_slab):
        return jnp.einsum('jb,bkl->jkl', window, ket_slab, precision=highest) + jnp.einsum('kc,jcl->jkl', window, ket_slab, precision=highest) + jnp.einsum('ld,jkd->jkl', coupling, ket_slab, precision=highest)
    others = lax.map(slab_terms, ket_slabs).reshape(tensor.shape)
    return -0.5 * (leading + others)

def krylov_step(vectors, image_vec, entries):
    correlation = jnp.stack([jnp.sum(vector * image_vec) for vector in vectors]) / entries
    residual = image_vec
    for position in range(len(vectors)):
        residual = residual - correlation[position] * vectors[position]
    length_value = jnp.sqrt(jnp.sum(residual * residual) / entries)
    return (correlation, length_value, residual / length_value)

def reference(density, decay_matrix, atom_order):
    coupling = decay_matrix[atom_order][:, atom_order]
    atom_count = coupling.shape[0]
    half = density.shape[1]
    entries = float(density.size)
    vector_one = density / jnp.sqrt(jnp.sum(density * density) / entries)
    coeff_one, length_one, vector_two = krylov_step([vector_one], liouvillian(vector_one, coupling), entries)
    coeff_two, length_two, next_vector = krylov_step([vector_one, vector_two], liouvillian(vector_two, coupling), entries)
    krylov_coeffs = jnp.concatenate([coeff_one, length_one[None], coeff_two, length_two[None]])
    jump_flux = jnp.einsum('ab,ajbl->jl', coupling[:, :half], density.reshape(atom_count, half, half, atom_count), precision=highest).reshape(-1) / atom_count
    return (next_vector, krylov_coeffs, jump_flux)
```

```python
import jax
import jax.numpy as jnp
from jax import lax
from jax.sharding import PartitionSpec as P

highest = lax.Precision.HIGHEST
both = ("ket", "blk")


def swap(rows):
    return lax.all_to_all(rows, both, split_axis=0, concat_axis=0, tiled=True)


def shards(density, decay_matrix, atom_order):
    pair_rows, bra_local, atom_count = density.shape
    blk = lax.axis_size("blk")
    devices = lax.axis_size("ket") * blk
    half = bra_local * blk
    own = half * atom_count // devices
    groups = atom_count // own
    entries = float(atom_count) * float(half) * float(half) * float(atom_count)
    onehot = (atom_order[:, None] == jnp.arange(atom_count)[None, :]).astype(jnp.float32)
    coupling = jnp.dot(
        jnp.dot(onehot, decay_matrix, precision=highest), onehot.T, precision=highest
    )
    window = coupling[:half, :half]
    mean_full = jnp.trace(coupling) / atom_count
    mean_half = jnp.trace(window) / half
    full_zero = coupling - mean_full * jnp.eye(atom_count, dtype=jnp.float32)
    half_zero = window - mean_half * jnp.eye(half, dtype=jnp.float32)
    shift = 2.0 * (mean_full + mean_half)

    def outer_terms(turned):
        return jnp.einsum("ia,akl->ikl", full_zero, turned, precision=highest) + jnp.einsum(
            "kb,ibl->ikl", half_zero, turned, precision=highest
        )

    def inner_terms(tensor):
        return jnp.einsum("jb,bkl->jkl", half_zero, tensor, precision=highest) + jnp.einsum(
            "ld,jkd->jkl", full_zero, tensor, precision=highest
        )

    sent = density.reshape(half, bra_local, groups, own).transpose(0, 2, 1, 3)
    turned = swap(sent.reshape(devices, bra_local * own)).reshape(atom_count, half, own)
    jump_flux = jnp.einsum("ik,ikl->l", coupling[:, :half], turned, precision=highest) / atom_count
    once = outer_terms(turned)
    twice = outer_terms(once)
    packed = jnp.stack(
        [once.reshape(devices, bra_local * own), twice.reshape(devices, bra_local * own)], axis=1
    )
    returned = swap(packed).reshape(half, groups, 2, bra_local, own).transpose(2, 0, 3, 1, 4)
    returned = returned.reshape((2,) + density.shape)
    once, twice = returned[0], returned[1]
    image_one = once + inner_terms(density)
    image_two = twice + inner_terms(once + image_one)
    local = jnp.stack(
        [
            jnp.sum(density * density),
            jnp.sum(density * image_one),
            jnp.sum(image_one * image_one),
            jnp.sum(image_one * image_two),
            jnp.sum(image_two * image_two),
        ]
    )
    shared = swap(jnp.broadcast_to(local[None, :], (devices, local.shape[0])))
    mom = jnp.sum(shared, axis=0) / entries
    ratio = mom[1] / mom[0]
    gap = mom[2] - ratio * mom[1]
    theta = (mom[3] - 2.0 * ratio * mom[2] + ratio * ratio * mom[1]) / gap
    slope = ratio + theta
    offset = theta * ratio - gap / mom[0]
    size = jnp.sqrt(mom[4] - slope * mom[3] + offset * mom[2])
    next_vector = (image_two - slope * image_one + offset * density) / size
    b_one = 0.5 * jnp.sqrt(gap / mom[0])
    krylov_coeffs = jnp.stack(
        [
            -0.5 * (ratio + shift),
            b_one,
            b_one,
            -0.5 * (theta + shift),
            0.5 * size / jnp.sqrt(gap),
        ]
    )
    return (next_vector, krylov_coeffs, jump_flux)


def solution(mesh):
    return jax.shard_map(
        shards,
        mesh=mesh,
        in_specs=(P("ket", "blk", None), P(), P()),
        out_specs=(P("ket", "blk", None), P(), P(("ket", "blk"))),
        check_vma=False,
    )
```

```python
import functools

import jax
import jax.numpy as jnp
from jax import lax
from jax.experimental import pallas as pl
from jax.experimental.pallas import tpu as pltpu
from jax.sharding import Mesh, PartitionSpec as P

highest = lax.Precision.HIGHEST
ket_axes = ("zh", "zl", "y", "c")
swap_axes = ("c", "x", "zl", "y", "zh")
N, H, KB = 128, 64, 4
KL = H // KB
f32 = jnp.float32


def dot(a, b):
    return jnp.dot(a, b, precision=highest, preferred_element_type=f32)


def call(body, outs, *args, scratch=(), out_specs=None, name=None):
    vmem = pl.BlockSpec(memory_space=pltpu.VMEM)
    single = not isinstance(outs, list)
    outs_list = [outs] if single else list(outs)
    res = pl.pallas_call(
        body,
        out_shape=[jax.ShapeDtypeStruct(s, f32) for s in outs_list],
        in_specs=[vmem] * len(args),
        out_specs=[vmem] * len(outs_list),
        scratch_shapes=list(scratch),
        compiler_params=pltpu.CompilerParams(vmem_limit_bytes=40 * 2**20),
        name=name,
    )(*args)
    return res[0] if single else res


def prep_body(decay_ref, order_ref, turned_ref, nat_ref, til_ref, win_ref, rect_ref, shift_ref):
    decay = decay_ref[...]
    rows = lax.broadcasted_iota(jnp.int32, (N, N), 0)
    cols = lax.broadcasted_iota(jnp.int32, (N, N), 1)
    eye = (rows == cols).astype(f32)
    pick = (rows == order_ref[...]).astype(f32)
    pick_t = (rows == turned_ref[...]).astype(f32)
    nat = dot(pick.T, dot(decay, pick))
    til = dot(pick_t.T, dot(decay, pick_t))
    rect = dot(pick.T, dot(decay, pick_t))
    mean_full = jnp.sum(nat * eye) / N
    win = nat[:H, :H]
    mean_half = jnp.sum(win * eye[:H, :H]) / H
    nat_ref[...] = nat - mean_full * eye
    til_ref[...] = til - mean_full * eye
    win_ref[...] = win - mean_half * eye[:H, :H]
    rect_ref[...] = rect[:H, :]
    shift_ref[...] = jnp.full((1, N), 2.0 * (mean_full + mean_half), f32)


def send_body(x_ref, out_ref):
    for cb in range(8):
        out_ref[:, cb, :] = x_ref[cb * N : (cb + 1) * N, :].T


def middle_body(recv_ref, til_ref, win_ref, rect_ref, out_ref, flux_ref):
    parts = []
    for h in range(2):
        blocks = [
            recv_ref[:, kb, :, h, :].reshape(N, N).T.reshape(8, KL, N) for kb in range(KB)
        ]
        for j8 in range(8):
            parts.append(jnp.concatenate([b[j8] for b in blocks], axis=0))
    til, win = til_ref[...], win_ref[...]
    rect = rect_ref[...] * (1.0 / N)
    for c in range(16):
        flux_ref[c] = jnp.sum(parts[c] * rect, axis=0, keepdims=True)

    def outer(parts):
        tall = dot(jnp.concatenate(parts, axis=0), til)
        wide = dot(win, jnp.concatenate(parts, axis=1))
        return [
            tall[c * H : (c + 1) * H, :] + wide[:, c * N : (c + 1) * N] for c in range(16)
        ]

    for t in range(2):
        parts = outer(parts)
        for h in range(2):
            for kb in range(KB):
                block = jnp.concatenate(
                    [parts[h * 8 + j8][kb * KL : (kb + 1) * KL, :] for j8 in range(8)], axis=0
                )
                out_ref[:, kb, :, t * 2 + h, :] = block.T.reshape(2, 64, N)


def inner(src_ref, dst_ref, nat, win):
    wide = dot(win, jnp.concatenate([src_ref[pl.ds(k, H, stride=KL), :] for k in range(KL)], axis=1))
    for k in range(KL):
        dst_ref[pl.ds(k, H, stride=KL), :] = wide[:, k * N : (k + 1) * N]
    dst_ref[...] += dot(src_ref[...], nat)


def first_body(x_ref, nat_ref, win_ref, flux_ref, out_ref, pass_ref):
    pass_ref[...] = flux_ref[...]
    inner(x_ref, out_ref, nat_ref[...], win_ref[...])


def back_body(recv_ref, x_ref, rx_ref, nat_ref, win_ref, one_ref, two_ref, mom_ref, tmp_ref, res_ref):
    for cb in range(8):
        jg, h = divmod(cb, 2)
        rows = slice(cb * N, (cb + 1) * N)
        once = recv_ref[:, jg * 4 + h, :].T
        image = once + rx_ref[rows, :]
        one_ref[rows, :] = image
        tmp_ref[rows, :] = once + image
    inner(tmp_ref, res_ref, nat_ref[...], win_ref[...])
    sums = [jnp.zeros((8, N), f32) for _ in range(5)]
    for cb in range(8):
        jg, h = divmod(cb, 2)
        rows = slice(cb * N, (cb + 1) * N)
        two = recv_ref[:, jg * 4 + 2 + h, :].T + res_ref[rows, :]
        two_ref[rows, :] = two
        one, x = one_ref[rows, :], x_ref[rows, :]
        for q, (a, b) in enumerate([(x, x), (x, one), (one, one), (one, two), (two, two)]):
            sums[q] = sums[q] + jnp.sum((a * b).reshape(16, 8, N), axis=0)
    lane = lax.broadcasted_iota(jnp.int32, (1, N), 1)
    row = jnp.zeros((1, N), f32)
    for q in range(5):
        row = jnp.where(lane == q, jnp.sum(sums[q]), row)
    mom_ref[...] = jnp.broadcast_to(row[None], mom_ref.shape)


def relay_body(in_ref, out_ref):
    row = jnp.sum(in_ref[...], axis=0)
    out_ref[...] = jnp.broadcast_to(row[None], out_ref.shape)


def final_body(mom_ref, x_ref, one_ref, two_ref, shift_ref, out_ref, coef_ref, *, entries):
    row = jnp.sum(mom_ref[...], axis=0) / entries
    lane = lax.broadcasted_iota(jnp.int32, (1, N), 1)

    def mom(q):
        return jnp.broadcast_to(
            jnp.sum(jnp.where(lane == q, row, 0.0), axis=1, keepdims=True), (1, N)
        )

    m0, m1, m2, m3, m4 = [mom(q) for q in range(5)]
    shift = shift_ref[...]
    ratio = m1 / m0
    gap = m2 - ratio * m1
    theta = (m3 - 2.0 * ratio * m2 + ratio * ratio * m1) / gap
    slope = ratio + theta
    offset = theta * ratio - gap / m0
    size = jnp.sqrt(m4 - slope * m3 + offset * m2)
    b_one = 0.5 * jnp.sqrt(gap / m0)
    coefs = [
        -0.5 * (ratio + shift),
        b_one,
        b_one,
        -0.5 * (theta + shift),
        0.5 * size / jnp.sqrt(gap),
    ]
    line = jnp.zeros((1, N), f32)
    for q in range(5):
        line = jnp.where(lane == q, coefs[q], line)
    coef_ref[...] = line
    inv = 1.0 / size
    a, b = slope * inv, offset * inv
    out_ref[...] = two_ref[...] * inv - one_ref[...] * a + x_ref[...] * b


def swap(rows, axes=swap_axes):
    return lax.all_to_all(rows, axes, split_axis=0, concat_axis=0, tiled=True)


def shards(density, decay_matrix, atom_order):
    entries = float(N) * float(H) * float(H) * float(N)
    x = density.reshape(H * KL, N)
    turned_order = atom_order.reshape(4, 16, 2).transpose(2, 1, 0).reshape(1, N)
    nat, til, win, rect, shift = call(
        prep_body,
        [(N, N), (N, N), (H, H), (H, N), (1, N)],
        decay_matrix,
        atom_order.reshape(1, N),
        turned_order,
        name="prep",
    )
    sent = call(send_body, (N, 8, N), x, name="send")
    recv = swap(sent.reshape(512, 2, N)).reshape(2, KB, 64, 2, N)
    back, flux = call(
        middle_body, [(2, KB, 64, 4, N), (16, 1, N)], recv, til, win, rect, name="middle"
    )
    returned = swap(back.reshape(512, 4, N)).reshape(N, 16, N)
    rx, flux = call(first_body, [(H * KL, N), (16, 1, N)], x, nat, win, flux, name="first")
    flux = swap(flux, ("zl", "y"))
    returned, rx, flux = lax.optimization_barrier((returned, rx, flux))
    one, two, mom = call(
        back_body,
        [(H * KL, N), (H * KL, N), (32, 1, N)],
        returned,
        x,
        rx,
        nat,
        win,
        scratch=[pltpu.VMEM((H * KL, N), f32), pltpu.VMEM((H * KL, N), f32)],
        name="back",
    )
    mom = swap(mom, ("zh", "zl", "x"))
    mom = call(relay_body, (16, 1, N), mom, name="relay")
    mom = swap(mom, ("y", "c"))
    out, coef = call(
        functools.partial(final_body, entries=entries),
        [(H * KL, N), (1, N)],
        mom,
        x,
        one,
        two,
        shift,
        name="final",
    )
    return (out.reshape(density.shape), coef[0, :5], jnp.sum(flux, axis=(1, 2)))


def solution(mesh):
    fine = Mesh(mesh.devices.reshape(4, 2, 8, 2, 4), ket_axes + ("x",))
    return jax.shard_map(
        shards,
        mesh=fine,
        in_specs=(P(ket_axes, "x", None), P(), P()),
        out_specs=(P(ket_axes, "x", None), P(), P(ket_axes + ("x",))),
        check_vma=False,
    )
```

```python
import functools

import jax
import jax.numpy as jnp
from jax import lax
from jax.experimental import pallas as pl
from jax.experimental.pallas import tpu as pltpu
from jax.sharding import Mesh, PartitionSpec as P

highest = lax.Precision.HIGHEST
ket_axes = ("zh", "zl", "y", "c")
swap_axes = ("c", "x", "zl", "y", "zh")
N, H, KB = 128, 64, 4
KL = H // KB
f32 = jnp.float32


def dot(a, b):
    return jnp.dot(a, b, precision=highest, preferred_element_type=f32)


def call(body, outs, *args, scratch=(), scalar=None, name=None):
    vmem = pl.BlockSpec(memory_space=pltpu.VMEM)
    in_specs = [vmem] * len(args)
    if scalar is not None:
        args = (scalar,) + args
        in_specs = [pl.BlockSpec(memory_space=pltpu.SMEM)] + in_specs
    single = not isinstance(outs, list)
    outs_list = [outs] if single else list(outs)
    res = pl.pallas_call(
        body,
        out_shape=[jax.ShapeDtypeStruct(s, f32) for s in outs_list],
        in_specs=in_specs,
        out_specs=[vmem] * len(outs_list),
        scratch_shapes=list(scratch),
        compiler_params=pltpu.CompilerParams(vmem_limit_bytes=40 * 2**20),
        name=name,
    )(*args)
    return res[0] if single else res


def prep_body(decay_ref, order_ref, turned_ref, nat_ref, til_ref, win_ref, rect_ref, shift_ref):
    decay = decay_ref[...]
    rows = lax.broadcasted_iota(jnp.int32, (N, N), 0)
    cols = lax.broadcasted_iota(jnp.int32, (N, N), 1)
    eye = (rows == cols).astype(f32)
    pick = (rows == order_ref[...]).astype(f32)
    pick_t = (rows == turned_ref[...]).astype(f32)
    nat = dot(pick.T, dot(decay, pick))
    til = dot(pick_t.T, dot(decay, pick_t))
    rect = dot(pick.T, dot(decay, pick_t))
    mean_full = jnp.sum(nat * eye) / N
    win = nat[:H, :H]
    mean_half = jnp.sum(win * eye[:H, :H]) / H
    nat_ref[...] = nat - mean_full * eye
    til_ref[...] = til - mean_full * eye
    win_ref[...] = win - mean_half * eye[:H, :H]
    rect_ref[...] = rect[:H, :]
    shift_ref[...] = jnp.full((1, N), 2.0 * (mean_full + mean_half), f32)


def send_body(x_ref, out_ref):
    for cb in range(8):
        out_ref[:, cb, :] = x_ref[cb * N : (cb + 1) * N, :].T


def middle_body(recv_ref, til_ref, win_ref, rect_ref, out_ref, flux_ref):
    parts = []
    for h in range(2):
        blocks = [
            recv_ref[:, kb, :, h, :].reshape(N, N).T.reshape(8, KL, N) for kb in range(KB)
        ]
        for j8 in range(8):
            parts.append(jnp.concatenate([b[j8] for b in blocks], axis=0))
    til, win = til_ref[...], win_ref[...]
    rect = rect_ref[...] * (1.0 / N)
    for c in range(16):
        flux_ref[c] = jnp.sum(parts[c] * rect, axis=0, keepdims=True)

    def outer(parts):
        tall = dot(jnp.concatenate(parts, axis=0), til)
        wide = dot(win, jnp.concatenate(parts, axis=1))
        return [
            tall[c * H : (c + 1) * H, :] + wide[:, c * N : (c + 1) * N] for c in range(16)
        ]

    for t in range(2):
        parts = outer(parts)
        for h in range(2):
            for kb in range(KB):
                block = jnp.concatenate(
                    [parts[h * 8 + j8][kb * KL : (kb + 1) * KL, :] for j8 in range(8)], axis=0
                )
                out_ref[:, kb, :, t * 2 + h, :] = block.T.reshape(2, 64, N)


def inner(src_ref, dst_ref, nat, win):
    wide = dot(win, jnp.concatenate([src_ref[pl.ds(k, H, stride=KL), :] for k in range(KL)], axis=1))
    for k in range(KL):
        dst_ref[pl.ds(k, H, stride=KL), :] = wide[:, k * N : (k + 1) * N]
    dst_ref[...] += dot(src_ref[...], nat)


def first_body(x_ref, nat_ref, win_ref, out_ref):
    inner(x_ref, out_ref, nat_ref[...], win_ref[...])


def place(where):
    return where // 128, (where // 64) % 2, (where // 8) % 8, (where // 4) % 2, where % 4


def back_body(
    where_ref, recv_ref, x_ref, rx_ref, nat_ref, win_ref, flux_ref, one_ref, two_ref, mom_ref, tmp_ref, res_ref
):
    for cb in range(8):
        jg, h = divmod(cb, 2)
        rows = slice(cb * N, (cb + 1) * N)
        once = recv_ref[:, jg * 4 + h, :].T
        image = once + rx_ref[rows, :]
        one_ref[rows, :] = image
        tmp_ref[rows, :] = once + image
    inner(tmp_ref, res_ref, nat_ref[...], win_ref[...])
    sums = [jnp.zeros((8, N), f32) for _ in range(5)]
    for cb in range(8):
        jg, h = divmod(cb, 2)
        rows = slice(cb * N, (cb + 1) * N)
        two = recv_ref[:, jg * 4 + 2 + h, :].T + res_ref[rows, :]
        two_ref[rows, :] = two
        one, x = one_ref[rows, :], x_ref[rows, :]
        for q, (a, b) in enumerate([(x, x), (x, one), (one, one), (one, two), (two, two)]):
            sums[q] = sums[q] + jnp.sum((a * b).reshape(16, 8, N), axis=0)
    lane = lax.broadcasted_iota(jnp.int32, (1, N), 1)
    row = jnp.zeros((1, N), f32)
    for q in range(5):
        row = jnp.where(lane == q, jnp.sum(sums[q]), row)
    zh, zl, _, _, xi = place(where_ref[0])
    flux = jnp.sum(flux_ref[...].reshape(16, N), axis=1, keepdims=True)
    spot = lax.broadcasted_iota(jnp.int32, (8, N), 1) == (
        lax.broadcasted_iota(jnp.int32, (8, N), 0) + 8 + 8 * zl
    )
    dest = lax.broadcasted_iota(jnp.int32, (4, 1, N), 0)
    for group in range(2):
        mine = jnp.sum(
            jnp.where(spot, flux[8 * group : 8 * group + 8], 0.0), axis=0, keepdims=True
        )
        for q in range(4):
            kept = jnp.where((dest == xi) & (zh == q), mine[None], 0.0)
            mom_ref[pl.ds(q * 8 + group * 4, 4)] = row[None] + kept


def relay_body(in_ref, out_ref):
    row = jnp.sum(in_ref[...], axis=0)
    out_ref[...] = jnp.broadcast_to(row[None], out_ref.shape)


def final_body(
    where_ref, mom_ref, x_ref, one_ref, two_ref, shift_ref, out_ref, coef_ref, flux_ref, *, entries
):
    got = mom_ref[...].reshape(16, N)
    _, _, y, c, _ = place(where_ref[0])
    lanes = lax.broadcasted_iota(jnp.int32, (16, N), 1)
    source = lax.broadcasted_iota(jnp.int32, (16, N), 0)
    flux = jnp.zeros((1, N), f32)
    for zl in range(2):
        entry = jnp.sum(
            jnp.where((lanes == 8 + 8 * zl + y) & (source % 2 == c), got, 0.0),
            axis=1,
            keepdims=True,
        )
        flux += jnp.sum(
            jnp.where(lanes == 8 * zl + source // 2, entry, 0.0), axis=0, keepdims=True
        )
    flux_ref[...] = flux[:, :16]
    row = jnp.sum(got, axis=0, keepdims=True) / entries
    lane = lax.broadcasted_iota(jnp.int32, (1, N), 1)

    def mom(q):
        return jnp.broadcast_to(
            jnp.sum(jnp.where(lane == q, row, 0.0), axis=1, keepdims=True), (1, N)
        )

    m0, m1, m2, m3, m4 = [mom(q) for q in range(5)]
    shift = shift_ref[...]
    ratio = m1 / m0
    gap = m2 - ratio * m1
    theta = (m3 - 2.0 * ratio * m2 + ratio * ratio * m1) / gap
    slope = ratio + theta
    offset = theta * ratio - gap / m0
    size = jnp.sqrt(m4 - slope * m3 + offset * m2)
    b_one = 0.5 * jnp.sqrt(gap / m0)
    coefs = [
        -0.5 * (ratio + shift),
        b_one,
        b_one,
        -0.5 * (theta + shift),
        0.5 * size / jnp.sqrt(gap),
    ]
    line = jnp.zeros((1, N), f32)
    for q in range(5):
        line = jnp.where(lane == q, coefs[q], line)
    coef_ref[...] = line[:, :5]
    inv = 1.0 / size
    a, b = slope * inv, offset * inv
    out_ref[...] = two_ref[...] * inv - one_ref[...] * a + x_ref[...] * b


def swap(rows, axes=swap_axes):
    return lax.all_to_all(rows, axes, split_axis=0, concat_axis=0, tiled=True)


def shards(density, decay_matrix, atom_order):
    entries = float(N) * float(H) * float(H) * float(N)
    x = density.reshape(H * KL, N)
    turned_order = atom_order.reshape(4, 16, 2).transpose(2, 1, 0).reshape(1, N)
    nat, til, win, rect, shift = call(
        prep_body,
        [(N, N), (N, N), (H, H), (H, N), (1, N)],
        decay_matrix,
        atom_order.reshape(1, N),
        turned_order,
        name="prep",
    )
    where = lax.axis_index(ket_axes + ("x",)).astype(jnp.int32).reshape(1)
    sent = call(send_body, (N, 8, N), x, name="send")
    recv = swap(sent.reshape(512, 2, N)).reshape(2, KB, 64, 2, N)
    rx = call(first_body, (H * KL, N), x, nat, win, name="first")
    recv, rx, where = lax.optimization_barrier((recv, rx, where))
    back, flux = call(
        middle_body, [(2, KB, 64, 4, N), (16, 1, N)], recv, til, win, rect, name="middle"
    )
    returned = swap(back.reshape(512, 4, N)).reshape(N, 16, N)
    one, two, mom = call(
        back_body,
        [(H * KL, N), (H * KL, N), (32, 1, N)],
        returned,
        x,
        rx,
        nat,
        win,
        flux,
        scratch=[pltpu.VMEM((H * KL, N), f32), pltpu.VMEM((H * KL, N), f32)],
        scalar=where,
        name="back",
    )
    mom = swap(mom, ("zh", "zl", "x"))
    mom = call(relay_body, (16, 1, N), mom, name="relay")
    mom = swap(mom, ("y", "c"))
    out, coef, flux = call(
        functools.partial(final_body, entries=entries),
        [(H * KL, N), (1, 5), (1, 16)],
        mom,
        x,
        one,
        two,
        shift,
        scalar=where,
        name="final",
    )
    return out.reshape(density.shape), coef.reshape(5), flux.reshape(16)


def solution(mesh):
    fine = Mesh(mesh.devices.reshape(4, 2, 8, 2, 4), ket_axes + ("x",))
    return jax.shard_map(
        shards,
        mesh=fine,
        in_specs=(P(ket_axes, "x", None), P(), P()),
        out_specs=(P(ket_axes, "x", None), P(), P(ket_axes + ("x",))),
        check_vma=False,
    )
```

```python
import functools

import jax
import jax.numpy as jnp
from jax import lax
from jax.experimental import pallas as pl
from jax.experimental.pallas import tpu as pltpu
from jax.sharding import Mesh, PartitionSpec as P

highest = lax.Precision.HIGHEST
ket_axes = ("zh", "zl", "y", "c")
swap_axes = ("c", "x", "zl", "y", "zh")
N, H, KB = 128, 64, 4
KL = H // KB
f32 = jnp.float32


def dot(a, b):
    return jnp.dot(a, b, precision=highest, preferred_element_type=f32)


def call(body, outs, *args, scratch=(), scalar=None, name=None, raw_in=False, raw_out=False):
    vmem = pl.BlockSpec(memory_space=pltpu.VMEM)
    raw = pl.BlockSpec(memory_space=pltpu.HBM)
    in_specs = [raw if raw_in else vmem] * len(args)
    if scalar is not None:
        args = (scalar,) + args
        in_specs = [pl.BlockSpec(memory_space=pltpu.SMEM)] + in_specs
    single = not isinstance(outs, list)
    outs_list = [outs] if single else list(outs)
    res = pl.pallas_call(
        body,
        out_shape=[jax.ShapeDtypeStruct(s, f32) for s in outs_list],
        in_specs=in_specs,
        out_specs=[raw if raw_out else vmem] + [vmem] * (len(outs_list) - 1),
        scratch_shapes=list(scratch),
        compiler_params=pltpu.CompilerParams(vmem_limit_bytes=40 * 2**20),
        name=name,
    )(*args)
    return res[0] if single else res


def prep_body(decay_ref, order_ref, turned_ref, nat_ref, til_ref, win_ref, rect_ref, shift_ref):
    decay = decay_ref[...]
    rows = lax.broadcasted_iota(jnp.int32, (N, N), 0)
    cols = lax.broadcasted_iota(jnp.int32, (N, N), 1)
    eye = (rows == cols).astype(f32)
    pick = (rows == order_ref[...]).astype(f32)
    pick_t = (rows == turned_ref[...]).astype(f32)
    nat = dot(pick.T, dot(decay, pick))
    til = dot(pick_t.T, dot(decay, pick_t))
    rect = dot(pick.T, dot(decay, pick_t))
    mean_full = jnp.sum(nat * eye) / N
    win = nat[:H, :H]
    mean_half = jnp.sum(win * eye[:H, :H]) / H
    nat_ref[...] = nat - mean_full * eye
    til_ref[...] = til - mean_full * eye
    win_ref[...] = win - mean_half * eye[:H, :H]
    rect_ref[...] = rect[:H, :]
    shift_ref[...] = jnp.full((1, N), 2.0 * (mean_full + mean_half), f32)


def send_body(x_ref, out_ref, buf_ref, sem):
    copies = []
    for cb in range(8):
        rows = pl.ds(cb * N, N)
        copies.append(pltpu.make_async_copy(x_ref.at[rows], buf_ref.at[rows], sem.at[cb]))
        copies[-1].start()
    for cb in range(8):
        copies[cb].wait()
        out_ref[:, cb, :] = buf_ref[cb * N : (cb + 1) * N, :].T


def middle_body(recv_ref, til_ref, win_ref, rect_ref, out_ref, flux_ref):
    parts = []
    for h in range(2):
        blocks = [
            recv_ref[:, kb, :, h, :].reshape(N, N).T.reshape(8, KL, N) for kb in range(KB)
        ]
        for j8 in range(8):
            parts.append(jnp.concatenate([b[j8] for b in blocks], axis=0))
    til, win = til_ref[...], win_ref[...]
    rect = rect_ref[...] * (1.0 / N)
    for c in range(16):
        flux_ref[c] = jnp.sum(parts[c] * rect, axis=0, keepdims=True)

    def outer(parts):
        tall = dot(jnp.concatenate(parts, axis=0), til)
        wide = dot(win, jnp.concatenate(parts, axis=1))
        return [
            tall[c * H : (c + 1) * H, :] + wide[:, c * N : (c + 1) * N] for c in range(16)
        ]

    for t in range(2):
        parts = outer(parts)
        for h in range(2):
            for kb in range(KB):
                block = jnp.concatenate(
                    [parts[h * 8 + j8][kb * KL : (kb + 1) * KL, :] for j8 in range(8)], axis=0
                )
                out_ref[:, kb, :, t * 2 + h, :] = block.T.reshape(2, 64, N)


def inner(src_ref, dst_ref, nat, win):
    wide = dot(win, jnp.concatenate([src_ref[pl.ds(k, H, stride=KL), :] for k in range(KL)], axis=1))
    for k in range(KL):
        dst_ref[pl.ds(k, H, stride=KL), :] = wide[:, k * N : (k + 1) * N]
    dst_ref[...] += dot(src_ref[...], nat)


def first_body(x_ref, nat_ref, win_ref, out_ref):
    inner(x_ref, out_ref, nat_ref[...], win_ref[...])


def place(where):
    return where // 128, (where // 64) % 2, (where // 8) % 8, (where // 4) % 2, where % 4


def back_body(
    where_ref, recv_ref, x_ref, rx_ref, nat_ref, win_ref, flux_ref, one_ref, two_ref, mom_ref, tmp_ref, res_ref
):
    for cb in range(8):
        jg, h = divmod(cb, 2)
        rows = slice(cb * N, (cb + 1) * N)
        once = recv_ref[:, jg * 4 + h, :].T
        image = once + rx_ref[rows, :]
        one_ref[rows, :] = image
        tmp_ref[rows, :] = once + image
    inner(tmp_ref, res_ref, nat_ref[...], win_ref[...])
    sums = [jnp.zeros((8, N), f32) for _ in range(5)]
    for cb in range(8):
        jg, h = divmod(cb, 2)
        rows = slice(cb * N, (cb + 1) * N)
        two = recv_ref[:, jg * 4 + 2 + h, :].T + res_ref[rows, :]
        two_ref[rows, :] = two
        one, x = one_ref[rows, :], x_ref[rows, :]
        for q, (a, b) in enumerate([(x, x), (x, one), (one, one), (one, two), (two, two)]):
            sums[q] = sums[q] + jnp.sum((a * b).reshape(16, 8, N), axis=0)
    lane = lax.broadcasted_iota(jnp.int32, (1, N), 1)
    row = jnp.zeros((1, N), f32)
    for q in range(5):
        row = jnp.where(lane == q, jnp.sum(sums[q]), row)
    zh, zl, _, _, xi = place(where_ref[0])
    flux = jnp.sum(flux_ref[...].reshape(16, N), axis=1, keepdims=True)
    spot = lax.broadcasted_iota(jnp.int32, (8, N), 1) == (
        lax.broadcasted_iota(jnp.int32, (8, N), 0) + 8 + 8 * zl
    )
    dest = lax.broadcasted_iota(jnp.int32, (4, 1, N), 0)
    for group in range(2):
        mine = jnp.sum(
            jnp.where(spot, flux[8 * group : 8 * group + 8], 0.0), axis=0, keepdims=True
        )
        for q in range(4):
            kept = jnp.where((dest == xi) & (zh == q), mine[None], 0.0)
            mom_ref[pl.ds(q * 8 + group * 4, 4)] = row[None] + kept


def relay_body(in_ref, out_ref):
    row = jnp.sum(in_ref[...], axis=0)
    out_ref[...] = jnp.broadcast_to(row[None], out_ref.shape)


def final_body(
    where_ref,
    mom_ref,
    x_ref,
    one_ref,
    two_ref,
    shift_ref,
    out_ref,
    coef_ref,
    flux_ref,
    buf_ref,
    sem,
    *,
    entries,
):
    got = mom_ref[...].reshape(16, N)
    row = jnp.sum(got, axis=0, keepdims=True) / entries
    lane = lax.broadcasted_iota(jnp.int32, (1, N), 1)

    def mom(q):
        return jnp.broadcast_to(
            jnp.sum(jnp.where(lane == q, row, 0.0), axis=1, keepdims=True), (1, N)
        )

    m0, m1, m2, m3, m4 = [mom(q) for q in range(5)]
    shift = shift_ref[...]
    ratio = m1 / m0
    gap = m2 - ratio * m1
    theta = (m3 - 2.0 * ratio * m2 + ratio * ratio * m1) / gap
    slope = ratio + theta
    offset = theta * ratio - gap / m0
    size = jnp.sqrt(m4 - slope * m3 + offset * m2)
    b_one = 0.5 * jnp.sqrt(gap / m0)
    coefs = [
        -0.5 * (ratio + shift),
        b_one,
        b_one,
        -0.5 * (theta + shift),
        0.5 * size / jnp.sqrt(gap),
    ]
    inv = 1.0 / size
    a, b = slope * inv, offset * inv
    copies = []
    for cb in range(4):
        rows = pl.ds(cb * 2 * N, 2 * N)
        buf_ref[rows, :] = two_ref[rows, :] * inv - one_ref[rows, :] * a + x_ref[rows, :] * b
        copies.append(pltpu.make_async_copy(buf_ref.at[rows], out_ref.at[rows], sem.at[cb]))
        copies[-1].start()
    line = jnp.zeros((1, N), f32)
    for q in range(5):
        line = jnp.where(lane == q, coefs[q], line)
    coef_ref[...] = line[:, :5]
    _, _, y, c, _ = place(where_ref[0])
    lanes = lax.broadcasted_iota(jnp.int32, (16, N), 1)
    source = lax.broadcasted_iota(jnp.int32, (16, N), 0)
    flux = jnp.zeros((1, N), f32)
    for zl in range(2):
        entry = jnp.sum(
            jnp.where((lanes == 8 + 8 * zl + y) & (source % 2 == c), got, 0.0),
            axis=1,
            keepdims=True,
        )
        flux += jnp.sum(
            jnp.where(lanes == 8 * zl + source // 2, entry, 0.0), axis=0, keepdims=True
        )
    flux_ref[...] = flux[:, :16]
    for copy in copies:
        copy.wait()


def swap(rows, axes=swap_axes):
    return lax.all_to_all(rows, axes, split_axis=0, concat_axis=0, tiled=True)


def shards(density, decay_matrix, atom_order):
    entries = float(N) * float(H) * float(H) * float(N)
    x = density.reshape(H * KL, N)
    turned_order = atom_order.reshape(4, 16, 2).transpose(2, 1, 0).reshape(1, N)
    nat, til, win, rect, shift = call(
        prep_body,
        [(N, N), (N, N), (H, H), (H, N), (1, N)],
        decay_matrix,
        atom_order.reshape(1, N),
        turned_order,
        name="prep",
    )
    where = lax.axis_index(ket_axes + ("x",)).astype(jnp.int32).reshape(1)
    sent = call(
        send_body,
        (N, 8, N),
        x,
        scratch=[pltpu.VMEM((H * KL, N), f32), pltpu.SemaphoreType.DMA((8,))],
        raw_in=True,
        name="send",
    )
    recv = swap(sent.reshape(512, 2, N)).reshape(2, KB, 64, 2, N)
    rx = call(first_body, (H * KL, N), x, nat, win, name="first")
    recv, rx, where = lax.optimization_barrier((recv, rx, where))
    back, flux = call(
        middle_body, [(2, KB, 64, 4, N), (16, 1, N)], recv, til, win, rect, name="middle"
    )
    returned = swap(back.reshape(512, 4, N)).reshape(N, 16, N)
    one, two, mom = call(
        back_body,
        [(H * KL, N), (H * KL, N), (32, 1, N)],
        returned,
        x,
        rx,
        nat,
        win,
        flux,
        scratch=[pltpu.VMEM((H * KL, N), f32), pltpu.VMEM((H * KL, N), f32)],
        scalar=where,
        name="back",
    )
    mom = swap(mom, ("zh", "zl", "x"))
    mom = call(relay_body, (16, 1, N), mom, name="relay")
    mom = swap(mom, ("y", "c"))
    out, coef, flux = call(
        functools.partial(final_body, entries=entries),
        [(H * KL, N), (1, 5), (1, 16)],
        mom,
        x,
        one,
        two,
        shift,
        scratch=[pltpu.VMEM((H * KL, N), f32), pltpu.SemaphoreType.DMA((4,))],
        scalar=where,
        raw_out=True,
        name="final",
    )
    return out.reshape(density.shape), coef.reshape(5), flux.reshape(16)


def solution(mesh):
    fine = Mesh(mesh.devices.reshape(4, 2, 8, 2, 4), ket_axes + ("x",))
    return jax.shard_map(
        shards,
        mesh=fine,
        in_specs=(P(ket_axes, "x", None), P(), P()),
        out_specs=(P(ket_axes, "x", None), P(), P(ket_axes + ("x",))),
        check_vma=False,
    )
```
